32 devices in a mesh: dp: 4 (over z), mp: 8 (over y, x, core).
Axes of the slice: x: 2, y: 2, z: 4, core: 2. Of those that a mesh axis runs over, the one named last changes fastest.
Arguments:
- grad_parts: bfloat16 [4, 8, 2, 18432, 128], P('dp', 'mp'), may hold values from -45 to 45
- master: float32 [8, 2, 18432, 128], P('mp', None, 'dp'), may hold values from -15 to 15
- momenta: float32 [3, 8, 2, 18432, 128], P(None, 'mp', None, 'dp'), may hold values from -45 to 45
- second: float32 [3, 8, 2, 18432, 128], P(None, 'mp', None, 'dp'), may hold values from 0.00025 to 330
- step_count: int32 [1], replicated, may hold values from 1 to 99999
- mlp_first: float32 [8, 4], replicated, may hold values from -2 to 2
- mlp_bias: float32 [4], replicated, may hold values from -3 to 3
- mlp_second: float32 [4, 2], replicated, may hold values from -3 to 3
- tensor_weight: float32 [10], replicated, may hold values from -2 to 2
Outputs:
- new_params: bfloat16 [8, 2, 18432, 128], P('mp')
- new_master: float32 [8, 2, 18432, 128], P('mp', None, 'dp')
- new_momenta: float32 [3, 8, 2, 18432, 128], P(None, 'mp', None, 'dp')
- new_second: float32 [3, 8, 2, 18432, 128], P(None, 'mp', None, 'dp')
- update: float32 [8, 2, 18432, 128], P('mp', None, 'dp')
The draws below stay inside these ranges and needn't reach their ends.
All inputs are finite; a program needn't handle non-finite values.
Results may differ from the reference program's by a relative error of at most 0.019.
Values may be sent and summed in bfloat16 or wider, within the bound.
A program may use at most 192 MiB of HBM per device.

```python
import jax
import jax.numpy as jnp
from jax import lax

D = 4608
HQ = 4096
LANES = 128
FEATS = 8
HIDDEN_UNITS = 4
NT = 2
ROWS = 18432
OWN = 4608
N_DP = 4
N_MP = 8


def texture(key):
    key_rows = jax.random.fold_in(key, 1)
    key_lanes = jax.random.fold_in(key, 2)
    key_blocks = jax.random.fold_in(key, 3)
    position = jnp.arange(N_MP, dtype=jnp.float32) / max(N_MP - 1, 1)
    rising = jnp.exp(jnp.log(3.0) * position)[:, None, None, None]
    owner = jnp.arange(N_DP, dtype=jnp.float32) / max(N_DP - 1, 1)
    owner_rise = jnp.exp(jnp.log(3.0) * (owner - 1.0))[None, None, :, None, None]
    owner_random = jnp.exp(jax.random.uniform(key_blocks, (N_MP, NT, N_DP, 1, 1), minval=-jnp.log(3.0), maxval=0.0))
    row_part = jnp.exp(jax.random.uniform(key_rows, (N_MP, NT, N_DP, OWN, 1), minval=0.0, maxval=jnp.log(5.0)))
    row_part = (row_part * owner_rise * owner_random).reshape(N_MP, NT, ROWS, 1)
    lane_part = jnp.exp(jax.random.uniform(key_lanes, (1, NT, 1, LANES), minval=0.0, maxval=jnp.log(2.0)))
    return rising * row_part * lane_part


def draw_grad_parts(key, part):
    scales = texture(jax.random.fold_in(key, 11))
    ratio = jnp.exp(jnp.log(3.0) * jnp.arange(N_DP, dtype=jnp.float32) / max(N_DP - 1, 1))[:, None, None, None, None]
    key_noise = jax.random.fold_in(key, 12)
    noise = jax.random.truncated_normal(key_noise, -5.0, 5.0, (N_DP, N_MP, NT, ROWS, LANES))
    values = 0.1 * ratio * scales * noise
    return values.astype(jnp.bfloat16)


def draw_master(key, part):
    scales = texture(jax.random.fold_in(key, 21))
    key_noise = jax.random.fold_in(key, 22)
    noise = jax.random.truncated_normal(key_noise, -5.0, 5.0, (N_MP, NT, ROWS, LANES))
    return 0.1 * scales * noise


def draw_momenta(key, part):
    scales = texture(jax.random.fold_in(key, 31))
    key_noise = jax.random.fold_in(key, 32)
    noise = jax.random.truncated_normal(key_noise, -5.0, 5.0, (3, N_MP, NT, ROWS, LANES))
    return 0.3 * scales[None] * noise


def draw_second(key, part):
    scales = texture(jax.random.fold_in(key, 41))
    key_noise = jax.random.fold_in(key, 42)
    factor = jnp.exp(jax.random.uniform(key_noise, (3, N_MP, NT, ROWS, LANES), minval=jnp.log(0.25), maxval=jnp.log(4.0)))
    base = 0.3 * scales
    return (base * base)[None] * factor


def centred(stream_key, extent, deviation, most, kind=jnp.bfloat16):
    result = jax.random.normal(stream_key, extent, jnp.float32) * deviation
    return jnp.minimum(jnp.maximum(result, -most), most).astype(kind)


def setup_inputs(seed: int = 0) -> dict:
    key_list = jax.random.split(jax.random.key(seed), 10)
    return {
        "grad_parts": draw_grad_parts(jax.random.fold_in(key_list[9], 71), 0),
        "master": draw_master(jax.random.fold_in(key_list[9], 71), 0),
        "momenta": draw_momenta(jax.random.fold_in(key_list[9], 71), 0),
        "second": draw_second(jax.random.fold_in(key_list[9], 71), 0),
        "step_count": jax.random.randint(key_list[4], (1,), 1, 100000).astype(jnp.int32),
        "mlp_first": centred(key_list[5], (FEATS, HIDDEN_UNITS), FEATS ** -0.5, 2.0, jnp.float32),
        "mlp_bias": centred(key_list[6], (HIDDEN_UNITS,), 0.5, 3.0, jnp.float32),
        "mlp_second": centred(key_list[7], (HIDDEN_UNITS, 2), HIDDEN_UNITS ** -0.5, 3.0, jnp.float32),
        "tensor_weight": centred(key_list[8], (FEATS + 2,), 0.3, 2.0, jnp.float32),
    }


RATES = (0.9, 0.99, 0.999)

def features_of(master, gradient, moments, squares):
    listing = [master, gradient, moments[0], moments[1], moments[2]]
    for slot_id in range(3):
        listing.append(moments[slot_id] / jnp.sqrt(squares[slot_id]))
    return listing

def perceptron(normed, boost, mlp_first, mlp_bias, mlp_second):
    direction = jnp.zeros_like(normed[0])
    magnitude = jnp.zeros_like(normed[0])
    for unit_id in range(mlp_first.shape[1]):
        active = mlp_first[0, unit_id] * normed[0]
        for feat_id in range(1, len(normed)):
            active = active + mlp_first[feat_id, unit_id] * normed[feat_id]
        active = jax.nn.relu(active + mlp_bias[unit_id])
        direction = direction + mlp_second[unit_id, 0] * active
        magnitude = magnitude + mlp_second[unit_id, 1] * active
    return direction * jnp.exp(0.5 * jnp.tanh(magnitude)) * boost

def tensor_boost(norms, step_count, tensor_weight):
    count = tensor_weight.shape[0] - 2
    step_value = step_count[0].astype(jnp.float32)
    first_phase = jnp.log1p(step_value) / 11.5
    second_phase = step_value / 100000.0
    logits = lax.optimization_barrier(jnp.sum(tensor_weight[:count, None] * jnp.log(norms), axis=0))
    logits = logits + tensor_weight[count] * first_phase + tensor_weight[count + 1] * second_phase
    return jnp.exp(jnp.tanh(logits))

def reference(grad_parts, master, momenta, second, step_count, mlp_first, mlp_bias, mlp_second, tensor_weight):
    gradient = lax.optimization_barrier(jnp.sum(grad_parts, axis=0, dtype=jnp.float32))
    new_momenta = jnp.stack([rate * momenta[i] + (1.0 - rate) * gradient for i, rate in enumerate(RATES)])
    new_second = jnp.stack([rate * second[i] + (1.0 - rate) * gradient * gradient for i, rate in enumerate(RATES)])
    listing = features_of(master, gradient, new_momenta, new_second)
    totals = jnp.stack([lax.optimization_barrier(jnp.sum(feature * feature, axis=(0, 2, 3))) for feature in listing])
    norms = jnp.sqrt(totals / float(D * HQ) + 1e-06)
    boost = tensor_boost(norms, step_count, tensor_weight)[None, :, None, None]
    normed = [listing[i] / norms[i][None, :, None, None] for i in range(len(listing))]
    update = perceptron(normed, boost, mlp_first, mlp_bias, mlp_second)
    new_master = master - 0.05 * update
    new_params = new_master.astype(jnp.bfloat16)
    return (new_params, new_master, new_momenta, new_second, update)
```

```python
import functools

import jax
import jax.numpy as jnp
from jax import lax
from jax.experimental import pallas as pl
from jax.experimental.pallas import tpu as pltpu
from jax.sharding import PartitionSpec as P

RATES = (0.9, 0.99, 0.999)
MESH = pl.DeviceIdType.MESH
STRIP = 32
LAG = 3
DEPTH = 4


def block_rows(rows, most=1152):
    best = STRIP
    for size in range(STRIP, most + 1, STRIP):
        if rows % size == 0:
            best = size
    return best


def advanced(g, momenta, second):
    moments = [b * m + (1.0 - b) * g for b, m in zip(RATES, momenta)]
    gg = g * g
    squares = [b * s + (1.0 - b) * gg for b, s in zip(RATES, second)]
    return moments, squares


def listing_of(master, g, moments, squares):
    ratios = [m * lax.rsqrt(s) for m, s in zip(moments, squares)]
    return [master, g, *moments, *ratios]


def update_of(listing, coef, base, feats, hidden):
    direction = None
    magnitude = None
    tail = base + feats * hidden
    for j in range(hidden):
        active = listing[0] * coef[base + j] + coef[tail + j]
        for f in range(1, feats):
            active = active + listing[f] * coef[base + f * hidden + j]
        active = jnp.maximum(active, 0.0)
        d = active * coef[tail + hidden + j]
        m = active * coef[tail + 2 * hidden + j]
        direction = d if direction is None else direction + d
        magnitude = m if magnitude is None else magnitude + m
    return direction * jnp.exp(0.5 * jnp.tanh(magnitude))


def pieces_of(own):
    strips = own // STRIP
    return max(k for k in range(1, 17) if strips % k == 0)


class Plan:
    def __init__(self, n_dp, n_mp, own):
        self.n, self.m, self.own = n_dp, n_mp, own
        self.k = pieces_of(own)
        self.pr = own // self.k
        self.lag = min(LAG, self.k)
        self.late = (2 * n_dp - 1) * self.k + max(0, self.lag + 8 - self.k)
        self.nt = self.late + self.k
        s0 = (n_dp - 2) * self.k + self.lag
        self.stats = (s0, s0 + (n_dp - 1) * self.k)
        self.send1 = tuple(s + self.k for s in self.stats)
        self.send2 = tuple(s + 2 for s in self.send1)
        self.done = tuple(s + 4 for s in self.send2)
        self.params = tuple(s + 1 for s in self.done)
        self.end = max(self.nt + self.lag * (n_dp - 1) + DEPTH, self.params[1] + self.k + 1)


def either(T, ticks):
    return (T == ticks[0]) | (T == ticks[1]), jnp.where(T >= ticks[1], 1, 0)


def within(T, starts, length):
    t = jnp.where(T >= starts[1], 1, 0)
    k = T - jnp.where(T >= starts[1], starts[1], starts[0])
    return (k >= 0) & (k < length), t, jnp.clip(k, 0, length - 1)


def mega_kernel(
    plan, feats, hidden,
    grad_ref, master_ref, mom_ref, sec_ref, step_ref, first_ref, bias_ref, second_ref, weight_ref,
    full_ref, p1_ref, right_ref, left_ref, g_ref, coef,
    gbuf, rbuf, masters, moms, secs, pbuf, acc, tot, near, nsum, far,
    load_sem, state_sem, send_sem, recv_sem, near_s, near_r, far_s, far_r, out_sem,
):
    n, m_n, own, K, pr = plan.n, plan.m, plan.own, plan.k, plan.pr
    width = (feats + 3) * hidden
    z = lax.axis_index("dp")
    m = lax.axis_index("mp")
    sides = (right_ref, left_ref)

    def chunk_load(t, c):
        rows = pl.ds(pl.multiple_of(c * own, STRIP), own)
        return pltpu.make_async_copy(grad_ref.at[0, 0, t, rows], gbuf.at[t, rows], load_sem.at[t, c])

    def state_loads(t):
        return (
            pltpu.make_async_copy(master_ref.at[0, t], masters.at[t], state_sem.at[t, 0]),
            pltpu.make_async_copy(mom_ref.at[:, 0, t], moms.at[t], state_sem.at[t, 1]),
            pltpu.make_async_copy(sec_ref.at[:, 0, t], secs.at[t], state_sem.at[t, 2]),
        )

    order = []
    for i in range((n + 1) // 2):
        order += [n - 1 - i] + ([i] if i != n - 1 - i else [])
    for t in range(2):
        for c in order:
            chunk_load(t, c).start()
    for t in range(2):
        for copy in state_loads(t):
            copy.start()

    barrier = pltpu.get_barrier_semaphore()
    for j in range(1, m_n):
        pl.semaphore_signal(barrier, inc=1, device_id=(z, lax.rem(m + j, m_n)), device_id_type=MESH)
    for j in range(1, n):
        pl.semaphore_signal(barrier, inc=1, device_id=(lax.rem(z + j, n), m), device_id_type=MESH)
    pl.semaphore_wait(barrier, m_n - 1 + n - 1)

    def place_of(d, T):
        q = z if d == 0 else n - 1 - z
        tau = T - plan.lag * q
        active = (tau >= 0) & (tau < plan.nt)
        tau = jnp.clip(tau, 0, plan.nt - 1)
        late = tau >= plan.late
        active = active & (late | (tau < (2 * n - 1) * K))
        s, k = lax.div(tau, K), lax.rem(jnp.where(late, tau - plan.late, tau), K)
        mid = (s >= n - 1) & (tau < (2 * n - 1) * K)
        cp = jnp.where(mid, 2 * n - 2 - s, jnp.where(late, q, n - 1 - s))
        t = jnp.where(mid, 1, 0)
        c = cp if d == 0 else n - 1 - cp
        si = jnp.clip(n - 1 - cp, 0, n - 2)
        return q, tau, active, k, mid, late, cp, t, c, si

    def piece(base, k):
        return pl.ds(pl.multiple_of(base + k * pr, STRIP), pr)

    def remote(d, src, dst, tau):
        to = lax.rem(z + 1, n) if d == 0 else lax.rem(z + n - 1, n)
        return pltpu.make_async_remote_copy(
            src_ref=src, dst_ref=dst, send_sem=send_sem.at[d, lax.rem(tau, DEPTH)], recv_sem=recv_sem.at[d, tau],
            device_id=(to, m), device_id_type=MESH,
        )

    def tick(T, carry):
        for d in range(2):
            q, tau, active, k, mid, late, cp, t, c, si = place_of(d, T)
            slot = rbuf.at[d, t, si, piece(0, k)]
            landed = full_ref.at[piece(c * own, k)]

            @pl.when(active & (q > 0) & (cp >= q) & ~late)
            def _():
                remote(d, slot, slot, tau).wait_recv()

            @pl.when(active & mid & (cp < q))
            def _():
                remote(d, landed, landed, tau).wait_recv()

            @pl.when(active & late & (q > 0))
            def _():
                remote(d, sides[d].at[piece(0, k)], sides[d].at[piece(0, k)], tau).wait_recv()

            @pl.when(active & (cp > q) & (k == 0))
            def _():
                chunk_load(t, c).wait()

            @pl.when(active & (q > 0) & (cp > q))
            def _():
                rows = piece(0, k)
                rbuf[d, t, si, rows, :] = rbuf[d, t, si, rows, :] + gbuf[t, piece(c * own, k), :]

        for d in range(2):
            q, tau, active, k, mid, late, cp, t, c, si = place_of(d, T - DEPTH)
            slot = rbuf.at[d, t, si, piece(0, k)]

            @pl.when(active & (q < n - 1) & ((cp > q) | mid | late))
            def _():
                remote(d, slot, slot, tau).wait_send()

            q, tau, active, k, mid, late, cp, t, c, si = place_of(d, T)
            slot = rbuf.at[d, t, si, piece(0, k)]
            landed = full_ref.at[piece(c * own, k)]

            @pl.when(active & (cp > q) & (q == 0))
            def _():
                remote(d, gbuf.at[t, piece(c * own, k)], slot, tau).start()

            @pl.when(active & (cp > q) & (q > 0))
            def _():
                remote(d, slot, slot, tau).start()

            @pl.when(active & mid & (cp == q) & (q < n - 1))
            def _():
                remote(d, pbuf.at[0, piece(0, k)], landed, tau).start()

            @pl.when(active & mid & (cp < q) & (q < n - 1))
            def _():
                remote(d, landed, landed, tau).start()

            @pl.when(active & late & (q < n - 1))
            def _():
                remote(d, pbuf.at[1, piece(0, k)], sides[d].at[piece(0, k)], tau).start()

        for d in range(2):
            edge = 0 if d == 0 else n - 1

            @pl.when((z == edge) & (T < K))
            def _():
                rows = piece(0, jnp.minimum(T, K - 1))
                for t in range(2):
                    rbuf[d, t, n - 2, rows, :] = jnp.zeros((pr, 128), jnp.bfloat16)

        live, t, k = within(T, plan.stats, K)

        @pl.when(live & (k == 0))
        def _():
            for copy in state_loads(t):
                copy.wait()
            chunk_load(t, z).wait()
            acc[...] = jnp.zeros_like(acc)

        @pl.when(live)
        def _():
            side = [jnp.minimum(n - 1 - z, n - 2), jnp.minimum(z, n - 2)]

            def body(i, sums):
                rows = pl.ds(pl.multiple_of(k * pr + i * STRIP, STRIP), STRIP)
                mine = pl.ds(pl.multiple_of(z * own + k * pr + i * STRIP, STRIP), STRIP)
                g = gbuf[t, mine, :].astype(jnp.float32)
                for d in range(2):
                    g = g + rbuf[d, t, side[d], rows, :].astype(jnp.float32)
                g = g.astype(jnp.bfloat16)
                gbuf[t, mine, :] = g
                g = g.astype(jnp.float32)
                moments, squares = advanced(
                    g, [moms[t, c, rows, :] for c in range(3)], [secs[t, c, rows, :] for c in range(3)]
                )
                listing = listing_of(masters[t, rows, :], g, moments, squares)
                return tuple(
                    a + jnp.sum((f * f).reshape(STRIP // 8, 8, 128), axis=0) for a, f in zip(sums, listing)
                )

            sums = lax.fori_loop(0, pr // STRIP, body, tuple(acc[f] for f in range(8)))
            for f in range(8):
                acc[f] = sums[f]

        @pl.when(live & (k == K - 1))
        def _():
            for f in range(8):
                tot[t, pl.ds(f, 1), :] = jnp.sum(acc[f], axis=0, keepdims=True)

        def near_copy(t, j):
            return pltpu.make_async_remote_copy(
                src_ref=tot.at[t], dst_ref=near.at[t, j], send_sem=near_s.at[t, j], recv_sem=near_r.at[t, j],
                device_id=(z, lax.rem(m + j, m_n)), device_id_type=MESH,
            )

        def far_copy(t, j):
            return pltpu.make_async_remote_copy(
                src_ref=nsum.at[t], dst_ref=far.at[t, j], send_sem=far_s.at[t, j], recv_sem=far_r.at[t, j],
                device_id=(lax.rem(z + j, n), m), device_id_type=MESH,
            )

        live, t = either(T, plan.send1)

        @pl.when(live)
        def _():
            for j in range(1, m_n):
                near_copy(t, j).start()

        live, t = either(T, tuple(s - 1 for s in plan.send2))

        @pl.when(live)
        def _():
            for j in range(1, m_n):
                near_copy(t, j).wait()
            total = tot[t]
            for j in range(1, m_n):
                total = total + near[t, j]
            nsum[t] = total

        live, t = either(T, plan.send2)

        @pl.when(live)
        def _():
            for j in range(1, n):
                far_copy(t, j).start()

        live, t = either(T, plan.done)

        @pl.when(live)
        def _():
            for j in range(1, n):
                far_copy(t, j).wait()
            total = nsum[t]
            for j in range(1, n):
                total = total + far[t, j]
            base = t * width
            sums = jnp.sum(total, axis=1, keepdims=True) + jnp.zeros((feats, 128), jnp.float32)
            norms = jnp.sqrt(sums / float(m_n * n * own * 128) + 1e-06)
            logs = jnp.log(norms)
            inverse = 1.0 / norms
            step = jnp.full((1, 128), step_ref[0].astype(jnp.float32))
            logits = weight_ref[feats] * (jnp.log(1.0 + step) / 11.5) + weight_ref[feats + 1] * (step / 100000.0)
            for f in range(feats):
                logits = logits + weight_ref[f] * logs[f : f + 1, :]
            boost = jnp.exp(jnp.tanh(logits))[0, 0]
            for f in range(feats):
                scale = inverse[f, 0]
                for j in range(hidden):
                    coef[base + f * hidden + j] = first_ref[j, f] * scale
            tail = base + feats * hidden
            for j in range(hidden):
                coef[tail + j] = bias_ref[j]
                coef[tail + hidden + j] = second_ref[0, j] * boost
                coef[tail + 2 * hidden + j] = second_ref[1, j]

        live, t, k = within(T, plan.params, K)

        @pl.when(live)
        def _():
            def body(i, carry):
                rows = pl.ds(pl.multiple_of(k * pr + i * STRIP, STRIP), STRIP)
                mine = pl.ds(pl.multiple_of(z * own + k * pr + i * STRIP, STRIP), STRIP)
                g = gbuf[t, mine, :].astype(jnp.float32)
                moments, squares = advanced(
                    g, [moms[t, c, rows, :] for c in range(3)], [secs[t, c, rows, :] for c in range(3)]
                )
                master = masters[t, rows, :]
                update = update_of(listing_of(master, g, moments, squares), coef, t * width, feats, hidden)
                pbuf[t, rows, :] = (master - 0.05 * update).astype(jnp.bfloat16)
                return carry

            lax.fori_loop(0, pr // STRIP, body, 0)

        @pl.when(T == plan.params[0] + K)
        def _():
            out(0).start()

        @pl.when(T == plan.params[1] + K)
        def _():
            out(3).start()

        for t in range(2):

            @pl.when(T == plan.stats[t] + K)
            def _():
                out(1 + t).start()

        return carry

    def out(i):
        mine = pl.ds(pl.multiple_of(z * own, STRIP), own)
        src, dst = (
            (pbuf.at[0], full_ref.at[mine]),
            (gbuf.at[0, mine], g_ref.at[0]),
            (gbuf.at[1, mine], g_ref.at[1]),
            (pbuf.at[1], p1_ref),
        )[i]
        return pltpu.make_async_copy(src, dst, out_sem.at[i])

    lax.fori_loop(0, plan.end, tick, 0)
    for i in range(4):
        out(i).wait()


def mega(n_dp, n_mp, grad_parts, master, momenta, second, step_count, mlp_first, mlp_bias, mlp_second, tensor_weight):
    feats, hidden = mlp_first.shape
    own, total_rows = master.shape[2], grad_parts.shape[3]
    plan = Plan(n_dp, n_mp, own)
    width = (feats + 3) * hidden
    smem = pl.BlockSpec(memory_space=pltpu.SMEM)
    anywhere = pl.BlockSpec(memory_space=pl.ANY)
    sem = pltpu.SemaphoreType.DMA
    return pl.pallas_call(
        functools.partial(mega_kernel, plan, feats, hidden),
        out_shape=(
            jax.ShapeDtypeStruct((total_rows, 128), jnp.bfloat16),
            jax.ShapeDtypeStruct((own, 128), jnp.bfloat16),
            jax.ShapeDtypeStruct((own, 128), jnp.bfloat16),
            jax.ShapeDtypeStruct((own, 128), jnp.bfloat16),
            jax.ShapeDtypeStruct((2, own, 128), jnp.bfloat16),
            jax.ShapeDtypeStruct((2 * width,), jnp.float32),
        ),
        in_specs=[anywhere] * 4 + [smem] * 5,
        out_specs=(anywhere,) * 5 + (smem,),
        scratch_shapes=[
            pltpu.VMEM((2, total_rows, 128), jnp.bfloat16),
            pltpu.VMEM((2, 2, n_dp - 1, own, 128), jnp.bfloat16),
            pltpu.VMEM((2, own, 128), jnp.float32),
            pltpu.VMEM((2, 3, own, 128), jnp.float32),
            pltpu.VMEM((2, 3, own, 128), jnp.float32),
            pltpu.VMEM((2, own, 128), jnp.bfloat16),
            pltpu.VMEM((8, 8, 128), jnp.float32),
            pltpu.VMEM((2, feats, 128), jnp.float32),
            pltpu.VMEM((2, n_mp, feats, 128), jnp.float32),
            pltpu.VMEM((2, feats, 128), jnp.float32),
            pltpu.VMEM((2, n_dp, feats, 128), jnp.float32),
            sem((2, n_dp)),
            sem((2, 3)),
            sem((2, DEPTH)),
            sem((2, plan.nt)),
            sem((2, n_mp)),
            sem((2, n_mp)),
            sem((2, n_dp)),
            sem((2, n_dp)),
            sem((4,)),
        ],
        compiler_params=pltpu.CompilerParams(
            collective_id=0, has_side_effects=True, vmem_limit_bytes=67_000_000
        ),
        cost_estimate=pl.CostEstimate(flops=10**9, bytes_accessed=10**8, transcendentals=0),
        name="exchange",
    )(grad_parts, master, momenta, second, step_count, mlp_first.T, mlp_bias, mlp_second.T, tensor_weight)


def finish_kernel(t, feats, hidden, width, coef, g_ref, master_ref, mom_ref, sec_ref, *rest):
    nm_ref, nmom_ref, nsec_ref, up_ref = rest[-4:]

    def body(k, carry):
        rows = pl.ds(pl.multiple_of(k * STRIP, STRIP), STRIP)
        g = g_ref[0, rows, :].astype(jnp.float32)
        moments, squares = advanced(
            g, [mom_ref[c, 0, 0, rows, :] for c in range(3)], [sec_ref[c, 0, 0, rows, :] for c in range(3)]
        )
        for c in range(3):
            nmom_ref[c, 0, 0, rows, :] = moments[c]
            nsec_ref[c, 0, 0, rows, :] = squares[c]
        master = master_ref[0, 0, rows, :]
        update = update_of(listing_of(master, g, moments, squares), coef, t * width, feats, hidden)
        up_ref[0, 0, rows, :] = update
        nm_ref[0, 0, rows, :] = master - 0.05 * update
        return carry

    lax.fori_loop(0, g_ref.shape[1] // STRIP, body, 0)


def finish(t, feats, hidden, coefs, g, master, momenta, second, earlier=()):
    own = g.shape[1]
    rows = block_rows(own)
    specs = [
        pl.BlockSpec((1, 1, rows, 128), lambda i: (0, t, i, 0)),
        pl.BlockSpec((3, 1, 1, rows, 128), lambda i: (0, 0, t, i, 0)),
        pl.BlockSpec((3, 1, 1, rows, 128), lambda i: (0, 0, t, i, 0)),
    ]
    return pl.pallas_call(
        functools.partial(finish_kernel, t, feats, hidden, coefs.shape[0] // 2),
        grid=(own // rows,),
        out_shape=(
            jax.ShapeDtypeStruct(master.shape, jnp.float32),
            jax.ShapeDtypeStruct(momenta.shape, jnp.float32),
            jax.ShapeDtypeStruct(second.shape, jnp.float32),
            jax.ShapeDtypeStruct(master.shape, jnp.float32),
        ),
        in_specs=[
            pl.BlockSpec(memory_space=pltpu.SMEM),
            pl.BlockSpec((1, rows, 128), lambda i: (t, i, 0)),
        ]
        + specs
        + [pl.BlockSpec(memory_space=pl.ANY)] * len(earlier),
        out_specs=(specs[0], specs[1], specs[2], specs[0]),
        input_output_aliases={5 + i: i for i in range(len(earlier))},
        cost_estimate=pl.CostEstimate(
            flops=own * 128 * 130, bytes_accessed=own * 128 * 62, transcendentals=5 * own * 128
        ),
        name=f"finish{t}",
    )(coefs, g, master, momenta, second, *earlier)


def assemble_kernel(n_dp, own, full_ref, mine_ref, *rest):
    count = 2 * (n_dp - 2)
    others = rest[:count]
    out_ref, fbuf, buf, load_sem, store_sem = rest[count:]
    z = lax.axis_index("dp")
    moves = [(full_ref, fbuf, out_ref.at[0, 0], None)]
    moves.append((mine_ref, buf.at[0], out_ref.at[0, 1, pl.ds(pl.multiple_of(z * own, STRIP), own)], None))
    for i in range(count):
        c = z - (i // 2 + 1) if i % 2 == 0 else z + (i // 2 + 1)
        ok = (c >= 0) if i % 2 == 0 else (c < n_dp)
        at = pl.ds(pl.multiple_of(jnp.clip(c, 0, n_dp - 1) * own, STRIP), own)
        moves.append((others[i], buf.at[1 + i], out_ref.at[0, 1, at], ok))

    def each(act):
        for i, (src, mid, dst, ok) in enumerate(moves):
            load = pltpu.make_async_copy(src, mid, load_sem.at[i])
            store = pltpu.make_async_copy(mid, dst, store_sem.at[i])
            if ok is None:
                act(load, store)
            else:
                pl.when(ok)(functools.partial(act, load, store))

    each(lambda load, store: load.start())

    def forward(load, store):
        load.wait()
        store.start()

    each(forward)
    each(lambda load, store: store.wait())


def assemble(n_dp, full, mine, others):
    own = mine.shape[0]
    anywhere = pl.BlockSpec(memory_space=pl.ANY)
    count = 2 + len(others)
    return pl.pallas_call(
        functools.partial(assemble_kernel, n_dp, own),
        out_shape=jax.ShapeDtypeStruct((1, 2) + full.shape, full.dtype),
        in_specs=[anywhere] * count,
        out_specs=anywhere,
        scratch_shapes=[
            pltpu.VMEM(full.shape, full.dtype),
            pltpu.VMEM((count - 1,) + mine.shape, mine.dtype),
            pltpu.SemaphoreType.DMA((count,)),
            pltpu.SemaphoreType.DMA((count,)),
        ],
        cost_estimate=pl.CostEstimate(flops=10**7, bytes_accessed=4 * full.size, transcendentals=0),
        name="assemble",
    )(full, mine, *others)


def last_kernel(n_dp, own, right_ref, left_ref, _, out_ref, buf, sems):
    z = lax.axis_index("dp")
    for d, (src, row) in enumerate(((right_ref, 0), (left_ref, (n_dp - 1) * own))):

        @pl.when(z == (n_dp - 1 if d == 0 else 0))
        def _():
            load = pltpu.make_async_copy(src, buf, sems.at[0])
            load.start()
            load.wait()
            store = pltpu.make_async_copy(buf, out_ref.at[0, 1, pl.ds(row, own)], sems.at[1])
            store.start()
            store.wait()


def last(n_dp, right, left, out):
    anywhere = pl.BlockSpec(memory_space=pl.ANY)
    return pl.pallas_call(
        functools.partial(last_kernel, n_dp, right.shape[0]),
        out_shape=jax.ShapeDtypeStruct(out.shape, out.dtype),
        in_specs=[anywhere] * 3,
        out_specs=anywhere,
        input_output_aliases={2: 0},
        scratch_shapes=[pltpu.VMEM(right.shape, right.dtype), pltpu.SemaphoreType.DMA((2,))],
        name="last",
    )(right, left, out)


def local(
    n_dp, n_mp, grad_parts, master, momenta, second, step_count, mlp_first, mlp_bias, mlp_second, tensor_weight
):
    feats, hidden = mlp_first.shape
    full0, p1, right, left, g, coefs = mega(
        n_dp, n_mp, grad_parts, master, momenta, second, step_count, mlp_first, mlp_bias, mlp_second, tensor_weight
    )
    others = [right, left]
    state = ()
    for step in range(2, n_dp):
        sent = (right, left)
        right = lax.ppermute(sent[0], "dp", [(i, i + 1) for i in range(step - 1, n_dp - 1)])
        left = lax.ppermute(sent[1], "dp", [(i, i - 1) for i in range(1, n_dp - step + 1)])
        if step <= 3:
            state = finish(step - 2, feats, hidden, coefs, g, master, momenta, second, state)
        if step < n_dp - 1:
            right, left, state = lax.optimization_barrier((right, left, state))
            others += [right, left]
    out = last(n_dp, right, left, assemble(n_dp, full0, p1, others))
    return (out, *state)


def solution(mesh):
    placed = (
        P("dp", "mp", None, None, None),
        P("mp", None, "dp", None),
        P(None, "mp", None, "dp", None),
        P(None, "mp", None, "dp", None),
        P(),
        P(),
        P(),
        P(),
        P(),
    )
    return jax.shard_map(
        functools.partial(local, mesh.shape["dp"], mesh.shape["mp"]),
        mesh=mesh,
        in_specs=placed,
        out_specs=(
            P("mp", None, None, None),
            P("mp", None, "dp", None),
            P(None, "mp", None, "dp", None),
            P(None, "mp", None, "dp", None),
            P("mp", None, "dp", None),
        ),
        check_vma=False,
    )
```

```python
import functools

import jax
import jax.numpy as jnp
from jax import lax
from jax.experimental import pallas as pl
from jax.experimental.pallas import tpu as pltpu
from jax.sharding import PartitionSpec as P

RATES = (0.9, 0.99, 0.999)
MESH = pl.DeviceIdType.MESH
STRIP = 32
LAG = 3
DEPTH = 4
MOST = 16


def block_rows(rows, most=1152):
    best = STRIP
    for size in range(STRIP, most + 1, STRIP):
        if rows % size == 0:
            best = size
    return best


def advanced(g, momenta, second):
    moments = [b * m + (1.0 - b) * g for b, m in zip(RATES, momenta)]
    gg = g * g
    squares = [b * s + (1.0 - b) * gg for b, s in zip(RATES, second)]
    return moments, squares


def listing_of(master, g, moments, squares):
    ratios = [m * lax.rsqrt(s) for m, s in zip(moments, squares)]
    return [master, g, *moments, *ratios]


def update_of(listing, coef, base, feats, hidden):
    direction = None
    magnitude = None
    tail = base + feats * hidden
    for j in range(hidden):
        active = listing[0] * coef[base + j] + coef[tail + j]
        for f in range(1, feats):
            active = active + listing[f] * coef[base + f * hidden + j]
        active = jnp.maximum(active, 0.0)
        d = active * coef[tail + hidden + j]
        m = active * coef[tail + 2 * hidden + j]
        direction = d if direction is None else direction + d
        magnitude = m if magnitude is None else magnitude + m
    return direction * jnp.exp(0.5 * jnp.tanh(magnitude))


def pieces_of(own):
    strips = own // STRIP
    return max(k for k in range(1, MOST + 1) if strips % k == 0)


class Plan:
    def __init__(self, n_dp, n_mp, own):
        self.n, self.m, self.own = n_dp, n_mp, own
        self.k = pieces_of(own)
        self.pr = own // self.k
        self.lag = min(LAG, self.k)
        self.late = (2 * n_dp - 1) * self.k + max(0, self.lag + 8 - self.k)
        self.nt = self.late + self.k
        s0 = (n_dp - 2) * self.k + self.lag
        self.stats = (s0, s0 + (n_dp - 1) * self.k)
        self.send1 = tuple(s + self.k for s in self.stats)
        self.send2 = tuple(s + 2 for s in self.send1)
        self.done = tuple(s + 4 for s in self.send2)
        self.params = tuple(s + 1 for s in self.done)
        self.gathered = (2 * n_dp - 1) * self.k + self.lag * (n_dp - 1)
        self.end = max(self.nt + self.lag * (n_dp - 1) + DEPTH, self.params[1] + self.k + 1)


def either(T, ticks):
    return (T == ticks[0]) | (T == ticks[1]), jnp.where(T >= ticks[1], 1, 0)


def within(T, starts, length):
    t = jnp.where(T >= starts[1], 1, 0)
    k = T - jnp.where(T >= starts[1], starts[1], starts[0])
    return (k >= 0) & (k < length), t, jnp.clip(k, 0, length - 1)


def mega_kernel(
    plan, feats, hidden,
    grad_ref, master_ref, mom_ref, sec_ref, step_ref, first_ref, bias_ref, second_ref, weight_ref,
    full_ref, p1_ref, right_ref, left_ref, g_ref, coef,
    gbuf, rbuf, masters, moms, secs, fbuf, pbuf, acc, tot, near, nsum, far,
    load_sem, state_sem, send_sem, recv_sem, near_s, near_r, far_s, far_r, out_sem,
):
    n, m_n, own, K, pr = plan.n, plan.m, plan.own, plan.k, plan.pr
    width = (feats + 3) * hidden
    z = lax.axis_index("dp")
    m = lax.axis_index("mp")
    sides = (right_ref, left_ref)

    def landing(d, receiver):
        first = (receiver < n // 2) == (d == 0) if n == 4 else jnp.bool_(d == 0)
        return first, ~first

    def chunk_load(t, c):
        rows = pl.ds(pl.multiple_of(c * own, STRIP), own)
        return pltpu.make_async_copy(grad_ref.at[0, 0, t, rows], gbuf.at[t, rows], load_sem.at[t, c])

    def state_loads(t):
        return (
            pltpu.make_async_copy(master_ref.at[0, t], masters.at[t], state_sem.at[t, 0]),
            pltpu.make_async_copy(mom_ref.at[:, 0, t], moms.at[t], state_sem.at[t, 1]),
            pltpu.make_async_copy(sec_ref.at[:, 0, t], secs.at[t], state_sem.at[t, 2]),
        )

    order = []
    for i in range((n + 1) // 2):
        order += [n - 1 - i] + ([i] if i != n - 1 - i else [])
    for t in range(2):
        for c in order:
            chunk_load(t, c).start()
    for t in range(2):
        for copy in state_loads(t):
            copy.start()

    barrier = pltpu.get_barrier_semaphore()
    for j in range(1, m_n):
        pl.semaphore_signal(barrier, inc=1, device_id=(z, lax.rem(m + j, m_n)), device_id_type=MESH)
    for j in range(1, n):
        pl.semaphore_signal(barrier, inc=1, device_id=(lax.rem(z + j, n), m), device_id_type=MESH)
    pl.semaphore_wait(barrier, m_n - 1 + n - 1)

    def place_of(d, T):
        q = z if d == 0 else n - 1 - z
        tau = T - plan.lag * q
        active = (tau >= 0) & (tau < plan.nt)
        tau = jnp.clip(tau, 0, plan.nt - 1)
        late = tau >= plan.late
        active = active & (late | (tau < (2 * n - 1) * K))
        s, k = lax.div(tau, K), lax.rem(jnp.where(late, tau - plan.late, tau), K)
        mid = (s >= n - 1) & (tau < (2 * n - 1) * K)
        cp = jnp.where(mid, 2 * n - 2 - s, jnp.where(late, q, n - 1 - s))
        t = jnp.where(mid, 1, 0)
        c = cp if d == 0 else n - 1 - cp
        si = jnp.clip(n - 1 - cp, 0, n - 2)
        return q, tau, active, k, mid, late, cp, t, c, si

    def piece(base, k):
        return pl.ds(pl.multiple_of(base + k * pr, STRIP), pr)

    def remote(d, src, dst, tau):
        to = lax.rem(z + 1, n) if d == 0 else lax.rem(z + n - 1, n)
        return pltpu.make_async_remote_copy(
            src_ref=src, dst_ref=dst, send_sem=send_sem.at[d, lax.rem(tau, DEPTH)], recv_sem=recv_sem.at[d, tau],
            device_id=(to, m), device_id_type=MESH,
        )

    def tick(T, carry):
        for d in range(2):
            q, tau, active, k, mid, late, cp, t, c, si = place_of(d, T)
            slot = rbuf.at[d, t, si, piece(0, k)]
            landed = fbuf.at[piece(c * own, k)]

            @pl.when(active & (q > 0) & (cp >= q) & ~late)
            def _():
                remote(d, slot, slot, tau).wait_recv()

            @pl.when(active & mid & (cp < q))
            def _():
                remote(d, landed, landed, tau).wait_recv()

            for side, chosen in enumerate(landing(d, z)):

                @pl.when(active & late & (q > 0) & chosen)
                def _():
                    remote(d, sides[side].at[piece(0, k)], sides[side].at[piece(0, k)], tau).wait_recv()

            @pl.when(active & (cp > q) & (k == 0))
            def _():
                chunk_load(t, c).wait()

            @pl.when(active & (q > 0) & (cp > q))
            def _():
                rows = piece(0, k)
                rbuf[d, t, si, rows, :] = rbuf[d, t, si, rows, :] + gbuf[t, piece(c * own, k), :]

        for d in range(2):
            q, tau, active, k, mid, late, cp, t, c, si = place_of(d, T - DEPTH)
            slot = rbuf.at[d, t, si, piece(0, k)]

            @pl.when(active & (q < n - 1) & ((cp > q) | mid | late))
            def _():
                remote(d, slot, slot, tau).wait_send()

            q, tau, active, k, mid, late, cp, t, c, si = place_of(d, T)
            slot = rbuf.at[d, t, si, piece(0, k)]
            landed = fbuf.at[piece(c * own, k)]

            @pl.when(active & (cp > q) & (q == 0))
            def _():
                remote(d, gbuf.at[t, piece(c * own, k)], slot, tau).start()

            @pl.when(active & (cp > q) & (q > 0))
            def _():
                remote(d, slot, slot, tau).start()

            @pl.when(active & mid & (cp <= q) & (q < n - 1))
            def _():
                remote(d, landed, landed, tau).start()

            for side, chosen in enumerate(landing(d, z + 1 if d == 0 else z - 1)):

                @pl.when(active & late & (q < n - 1) & chosen)
                def _():
                    remote(d, pbuf.at[piece(0, k)], sides[side].at[piece(0, k)], tau).start()

        for d in range(2):
            edge = 0 if d == 0 else n - 1

            @pl.when((z == edge) & (T < K))
            def _():
                rows = piece(0, jnp.minimum(T, K - 1))
                for t in range(2):
                    rbuf[d, t, n - 2, rows, :] = jnp.zeros((pr, 128), jnp.bfloat16)

        live, t, k = within(T, plan.stats, K)

        @pl.when(live & (k == 0))
        def _():
            for copy in state_loads(t):
                copy.wait()
            chunk_load(t, z).wait()
            acc[...] = jnp.zeros_like(acc)

        @pl.when(live)
        def _():
            side = [jnp.minimum(n - 1 - z, n - 2), jnp.minimum(z, n - 2)]

            def body(i, sums):
                rows = pl.ds(pl.multiple_of(k * pr + i * STRIP, STRIP), STRIP)
                mine = pl.ds(pl.multiple_of(z * own + k * pr + i * STRIP, STRIP), STRIP)
                g = gbuf[t, mine, :].astype(jnp.float32)
                for d in range(2):
                    g = g + rbuf[d, t, side[d], rows, :].astype(jnp.float32)
                g = g.astype(jnp.bfloat16)
                gbuf[t, mine, :] = g
                g = g.astype(jnp.float32)
                moments, squares = advanced(
                    g, [moms[t, c, rows, :] for c in range(3)], [secs[t, c, rows, :] for c in range(3)]
                )
                listing = listing_of(masters[t, rows, :], g, moments, squares)
                return tuple(
                    a + jnp.sum((f * f).reshape(STRIP // 8, 8, 128), axis=0) for a, f in zip(sums, listing)
                )

            sums = lax.fori_loop(0, pr // STRIP, body, tuple(acc[f] for f in range(8)))
            for f in range(8):
                acc[f] = sums[f]

        @pl.when(live & (k == K - 1))
        def _():
            for f in range(8):
                tot[t, pl.ds(f, 1), :] = jnp.sum(acc[f], axis=0, keepdims=True)

        def near_copy(t, j):
            return pltpu.make_async_remote_copy(
                src_ref=tot.at[t], dst_ref=near.at[t, j], send_sem=near_s.at[t, j], recv_sem=near_r.at[t, j],
                device_id=(z, lax.rem(m + j, m_n)), device_id_type=MESH,
            )

        def far_copy(t, j):
            return pltpu.make_async_remote_copy(
                src_ref=nsum.at[t], dst_ref=far.at[t, j], send_sem=far_s.at[t, j], recv_sem=far_r.at[t, j],
                device_id=(lax.rem(z + j, n), m), device_id_type=MESH,
            )

        live, t = either(T, plan.send1)

        @pl.when(live)
        def _():
            for j in range(1, m_n):
                near_copy(t, j).start()

        live, t = either(T, tuple(s - 1 for s in plan.send2))

        @pl.when(live)
        def _():
            for j in range(1, m_n):
                near_copy(t, j).wait()
            total = tot[t]
            for j in range(1, m_n):
                total = total + near[t, j]
            nsum[t] = total

        live, t = either(T, plan.send2)

        @pl.when(live)
        def _():
            for j in range(1, n):
                far_copy(t, j).start()

        live, t = either(T, plan.done)

        @pl.when(live)
        def _():
            for j in range(1, n):
                far_copy(t, j).wait()
            total = nsum[t]
            for j in range(1, n):
                total = total + far[t, j]
            base = t * width
            sums = jnp.sum(total, axis=1, keepdims=True) + jnp.zeros((feats, 128), jnp.float32)
            norms = jnp.sqrt(sums / float(m_n * n * own * 128) + 1e-06)
            logs = jnp.log(norms)
            inverse = 1.0 / norms
            step = jnp.full((1, 128), step_ref[0].astype(jnp.float32))
            logits = weight_ref[feats] * (jnp.log(1.0 + step) / 11.5) + weight_ref[feats + 1] * (step / 100000.0)
            for f in range(feats):
                logits = logits + weight_ref[f] * logs[f : f + 1, :]
            boost = jnp.exp(jnp.tanh(logits))[0, 0]
            for f in range(feats):
                scale = inverse[f, 0]
                for j in range(hidden):
                    coef[base + f * hidden + j] = first_ref[j, f] * scale
            tail = base + feats * hidden
            for j in range(hidden):
                coef[tail + j] = bias_ref[j]
                coef[tail + hidden + j] = second_ref[0, j] * boost
                coef[tail + 2 * hidden + j] = second_ref[1, j]

        live, t, k = within(T, plan.params, K)

        def params(fresh, at):
            def body(i, carry):
                rows = pl.ds(pl.multiple_of(k * pr + i * STRIP, STRIP), STRIP)
                mine = pl.ds(pl.multiple_of(z * own + k * pr + i * STRIP, STRIP), STRIP)
                g = gbuf[t, mine, :].astype(jnp.float32)
                moments, squares = advanced(
                    g, [moms[t, c, rows, :] for c in range(3)], [secs[t, c, rows, :] for c in range(3)]
                )
                master = masters[t, rows, :]
                update = update_of(listing_of(master, g, moments, squares), coef, t * width, feats, hidden)
                to = pl.ds(pl.multiple_of(at + k * pr + i * STRIP, STRIP), STRIP)
                fresh[to, :] = (master - 0.05 * update).astype(jnp.bfloat16)
                return carry

            lax.fori_loop(0, pr // STRIP, body, 0)

        @pl.when(live & (t == 0))
        def _():
            params(fbuf, z * own)

        @pl.when(live & (t == 1))
        def _():
            params(pbuf, 0)

        @pl.when(T == plan.gathered)
        def _():
            out(0).start()

        @pl.when(T == plan.params[1] + K)
        def _():
            out(3).start()

        for t in range(2):

            @pl.when(T == plan.stats[t] + K)
            def _():
                out(1 + t).start()

        return carry

    def out(i):
        mine = pl.ds(pl.multiple_of(z * own, STRIP), own)
        src, dst = (
            (fbuf, full_ref),
            (gbuf.at[0, mine], g_ref.at[0]),
            (gbuf.at[1, mine], g_ref.at[1]),
            (pbuf, p1_ref),
        )[i]
        return pltpu.make_async_copy(src, dst, out_sem.at[i])

    lax.fori_loop(0, plan.end, tick, 0)
    for i in range(4):
        out(i).wait()


def mega(n_dp, n_mp, grad_parts, master, momenta, second, step_count, mlp_first, mlp_bias, mlp_second, tensor_weight):
    feats, hidden = mlp_first.shape
    own, total_rows = master.shape[2], grad_parts.shape[3]
    plan = Plan(n_dp, n_mp, own)
    width = (feats + 3) * hidden
    smem = pl.BlockSpec(memory_space=pltpu.SMEM)
    anywhere = pl.BlockSpec(memory_space=pl.ANY)
    sem = pltpu.SemaphoreType.DMA
    return pl.pallas_call(
        functools.partial(mega_kernel, plan, feats, hidden),
        out_shape=(
            jax.ShapeDtypeStruct((total_rows, 128), jnp.bfloat16),
            jax.ShapeDtypeStruct((own, 128), jnp.bfloat16),
            jax.ShapeDtypeStruct((own, 128), jnp.bfloat16),
            jax.ShapeDtypeStruct((own, 128), jnp.bfloat16),
            jax.ShapeDtypeStruct((2, own, 128), jnp.bfloat16),
            jax.ShapeDtypeStruct((2 * width,), jnp.float32),
        ),
        in_specs=[anywhere] * 4 + [smem] * 5,
        out_specs=(anywhere,) * 5 + (smem,),
        scratch_shapes=[
            pltpu.VMEM((2, total_rows, 128), jnp.bfloat16),
            pltpu.VMEM((2, 2, n_dp - 1, own, 128), jnp.bfloat16),
            pltpu.VMEM((2, own, 128), jnp.float32),
            pltpu.VMEM((2, 3, own, 128), jnp.float32),
            pltpu.VMEM((2, 3, own, 128), jnp.float32),
            pltpu.VMEM((total_rows, 128), jnp.bfloat16),
            pltpu.VMEM((own, 128), jnp.bfloat16),
            pltpu.VMEM((8, 8, 128), jnp.float32),
            pltpu.VMEM((2, feats, 128), jnp.float32),
            pltpu.VMEM((2, n_mp, feats, 128), jnp.float32),
            pltpu.VMEM((2, feats, 128), jnp.float32),
            pltpu.VMEM((2, n_dp, feats, 128), jnp.float32),
            sem((2, n_dp)),
            sem((2, 3)),
            sem((2, DEPTH)),
            sem((2, plan.nt)),
            sem((2, n_mp)),
            sem((2, n_mp)),
            sem((2, n_dp)),
            sem((2, n_dp)),
            sem((4,)),
        ],
        compiler_params=pltpu.CompilerParams(
            collective_id=0, has_side_effects=True, vmem_limit_bytes=67_000_000
        ),
        cost_estimate=pl.CostEstimate(flops=10**9, bytes_accessed=10**8, transcendentals=0),
        name="exchange",
    )(grad_parts, master, momenta, second, step_count, mlp_first.T, mlp_bias, mlp_second.T, tensor_weight)


def finish_kernel(t, feats, hidden, width, coef, g_ref, master_ref, mom_ref, sec_ref, *rest):
    nm_ref, nmom_ref, nsec_ref, up_ref = rest[-4:]

    def body(k, carry):
        rows = pl.ds(pl.multiple_of(k * STRIP, STRIP), STRIP)
        g = g_ref[0, rows, :].astype(jnp.float32)
        moments, squares = advanced(
            g, [mom_ref[c, 0, 0, rows, :] for c in range(3)], [sec_ref[c, 0, 0, rows, :] for c in range(3)]
        )
        for c in range(3):
            nmom_ref[c, 0, 0, rows, :] = moments[c]
            nsec_ref[c, 0, 0, rows, :] = squares[c]
        master = master_ref[0, 0, rows, :]
        update = update_of(listing_of(master, g, moments, squares), coef, t * width, feats, hidden)
        up_ref[0, 0, rows, :] = update
        nm_ref[0, 0, rows, :] = master - 0.05 * update
        return carry

    lax.fori_loop(0, g_ref.shape[1] // STRIP, body, 0)


def finish(t, feats, hidden, coefs, g, master, momenta, second, earlier=()):
    own = g.shape[1]
    rows = block_rows(own)
    specs = [
        pl.BlockSpec((1, 1, rows, 128), lambda i: (0, t, i, 0)),
        pl.BlockSpec((3, 1, 1, rows, 128), lambda i: (0, 0, t, i, 0)),
        pl.BlockSpec((3, 1, 1, rows, 128), lambda i: (0, 0, t, i, 0)),
    ]
    return pl.pallas_call(
        functools.partial(finish_kernel, t, feats, hidden, coefs.shape[0] // 2),
        grid=(own // rows,),
        out_shape=(
            jax.ShapeDtypeStruct(master.shape, jnp.float32),
            jax.ShapeDtypeStruct(momenta.shape, jnp.float32),
            jax.ShapeDtypeStruct(second.shape, jnp.float32),
            jax.ShapeDtypeStruct(master.shape, jnp.float32),
        ),
        in_specs=[
            pl.BlockSpec(memory_space=pltpu.SMEM),
            pl.BlockSpec((1, rows, 128), lambda i: (t, i, 0)),
        ]
        + specs
        + [pl.BlockSpec(memory_space=pl.ANY)] * len(earlier),
        out_specs=(specs[0], specs[1], specs[2], specs[0]),
        input_output_aliases={5 + i: i for i in range(len(earlier))},
        cost_estimate=pl.CostEstimate(
            flops=own * 128 * 130, bytes_accessed=own * 128 * 62, transcendentals=5 * own * 128
        ),
        name=f"finish{t}",
    )(coefs, g, master, momenta, second, *earlier)


def assemble_kernel(n_dp, own, chunks, full_ref, mine_ref, *rest):
    count = len(chunks)
    others = rest[:count]
    out_ref, fbuf, buf, load_sem, store_sem = rest[count:]
    z = lax.axis_index("dp")
    moves = [(full_ref, fbuf, out_ref.at[0, 0], None)]
    moves.append((mine_ref, buf.at[0], out_ref.at[0, 1, pl.ds(pl.multiple_of(z * own, STRIP), own)], None))
    for i, chunk in enumerate(chunks):
        c = chunk(z)
        at = pl.ds(pl.multiple_of(jnp.clip(c, 0, n_dp - 1) * own, STRIP), own)
        moves.append((others[i], buf.at[1 + i], out_ref.at[0, 1, at], (c >= 0) & (c < n_dp)))

    def each(act):
        for i, (src, mid, dst, ok) in enumerate(moves):
            def move(i=i, src=src, mid=mid, dst=dst):
                act(
                    functools.partial(pltpu.make_async_copy, src, mid, load_sem.at[i]),
                    functools.partial(pltpu.make_async_copy, mid, dst, store_sem.at[i]),
                )

            if ok is None:
                move()
            else:
                pl.when(ok)(move)

    each(lambda load, store: load().start())

    def forward(load, store):
        load().wait()
        store().start()

    each(forward)
    each(lambda load, store: store().wait())


def assemble(n_dp, full, mine, others, chunks):
    own = mine.shape[0]
    anywhere = pl.BlockSpec(memory_space=pl.ANY)
    count = 2 + len(others)
    return pl.pallas_call(
        functools.partial(assemble_kernel, n_dp, own, chunks),
        out_shape=jax.ShapeDtypeStruct((1, 2) + full.shape, full.dtype),
        in_specs=[anywhere] * count,
        out_specs=anywhere,
        scratch_shapes=[
            pltpu.VMEM(full.shape, full.dtype),
            pltpu.VMEM((count - 1,) + mine.shape, mine.dtype),
            pltpu.SemaphoreType.DMA((count,)),
            pltpu.SemaphoreType.DMA((count,)),
        ],
        cost_estimate=pl.CostEstimate(flops=10**7, bytes_accessed=4 * full.size, transcendentals=0),
        name="assemble",
    )(full, mine, *others)


def last_kernel(n_dp, own, *rest):
    out_ref, sem = rest[-2:]
    z = lax.axis_index("dp")
    for i, row in enumerate((0, (n_dp - 1) * own)):

        @pl.when(z == (n_dp - 1 if i == 0 else 0))
        def _():
            src = rest[0] if i == 0 else rest[len(rest) - 4]
            store = pltpu.make_async_copy(src, out_ref.at[0, 1, pl.ds(row, own)], sem)
            store.start()
            store.wait()


def last(n_dp, arrived, out):
    anywhere = pl.BlockSpec(memory_space=pl.ANY)
    return pl.pallas_call(
        functools.partial(last_kernel, n_dp, arrived[0].shape[0]),
        out_shape=jax.ShapeDtypeStruct(out.shape, out.dtype),
        in_specs=[anywhere] * (len(arrived) + 1),
        out_specs=anywhere,
        input_output_aliases={len(arrived): 0},
        scratch_shapes=[pltpu.SemaphoreType.DMA],
        compiler_params=pltpu.CompilerParams(vmem_limit_bytes=4 << 20),
        name="last",
    )(*arrived, out)


def local(
    n_dp, n_mp, grad_parts, master, momenta, second, step_count, mlp_first, mlp_bias, mlp_second, tensor_weight
):
    feats, hidden = mlp_first.shape
    full0, p1, right, left, g, coefs = mega(
        n_dp, n_mp, grad_parts, master, momenta, second, step_count, mlp_first, mlp_bias, mlp_second, tensor_weight
    )
    others = [right, left]
    net = (feats, hidden, coefs, g, master, momenta, second)
    if n_dp == 4:
        inner, outer = right, left
        crossed = lax.ppermute(inner, "dp", [(1, 2), (2, 1)])
        ended = lax.ppermute(outer, "dp", [(2, 3), (1, 0)])
        state = finish(0, *net)
        crossed, state = lax.optimization_barrier((crossed, state))
        arrived = [lax.ppermute(crossed, "dp", [(2, 3), (1, 0)])]
        state = finish(1, *net, state)
        others += [crossed, ended]
        none = -1
        chunks = [
            lambda z: jnp.where(z == 1, 0, jnp.where(z == 2, 3, none)),
            lambda z: jnp.where(z < 2, z + 1, z - 1),
            lambda z: jnp.where(z == 1, 3, jnp.where(z == 2, 0, none)),
            lambda z: jnp.where(z == 0, 2, jnp.where(z == 3, 1, none)),
        ]
    else:
        chunks = [lambda z: z - 1, lambda z: z + 1]
        state = ()
        for step in range(2, n_dp):
            sent = (right, left)
            right = lax.ppermute(sent[0], "dp", [(i, i + 1) for i in range(step - 1, n_dp - 1)])
            left = lax.ppermute(sent[1], "dp", [(i, i - 1) for i in range(1, n_dp - step + 1)])
            if step <= 3:
                state = finish(step - 2, *net, state)
            if step < n_dp - 1:
                right, left, state = lax.optimization_barrier((right, left, state))
                others += [right, left]
                chunks += [lambda z, step=step: z - step, lambda z, step=step: z + step]
        arrived = [right, left]
    out = last(n_dp, arrived, assemble(n_dp, full0, p1, others, chunks))
    return (out, *state)


def solution(mesh):
    placed = (
        P("dp", "mp", None, None, None),
        P("mp", None, "dp", None),
        P(None, "mp", None, "dp", None),
        P(None, "mp", None, "dp", None),
        P(),
        P(),
        P(),
        P(),
        P(),
    )
    return jax.shard_map(
        functools.partial(local, mesh.shape["dp"], mesh.shape["mp"]),
        mesh=mesh,
        in_specs=placed,
        out_specs=(
            P("mp", None, None, None),
            P("mp", None, "dp", None),
            P(None, "mp", None, "dp", None),
            P(None, "mp", None, "dp", None),
            P("mp", None, "dp", None),
        ),
        check_vma=False,
    )
```

```python
import functools

import jax
import jax.numpy as jnp
from jax import lax
from jax.experimental import pallas as pl
from jax.experimental.pallas import tpu as pltpu
from jax.sharding import PartitionSpec as P

RATES = (0.9, 0.99, 0.999)
MESH = pl.DeviceIdType.MESH
STRIP = 32
LAG = 3
DEPTH = 4
MOST = 16
BLOCK = 1152


def block_rows(rows, most=1152):
    best = STRIP
    for size in range(STRIP, most + 1, STRIP):
        if rows % size == 0:
            best = size
    return best


def advanced(g, momenta, second):
    moments = [b * m + (1.0 - b) * g for b, m in zip(RATES, momenta)]
    gg = g * g
    squares = [b * s + (1.0 - b) * gg for b, s in zip(RATES, second)]
    return moments, squares


def listing_of(master, g, moments, squares):
    ratios = [m * lax.rsqrt(s) for m, s in zip(moments, squares)]
    return [master, g, *moments, *ratios]


def update_of(listing, coef, base, feats, hidden):
    direction = None
    magnitude = None
    tail = base + feats * hidden
    for j in range(hidden):
        active = listing[0] * coef[base + j] + coef[tail + j]
        for f in range(1, feats):
            active = active + listing[f] * coef[base + f * hidden + j]
        active = jnp.maximum(active, 0.0)
        d = active * coef[tail + hidden + j]
        m = active * coef[tail + 2 * hidden + j]
        direction = d if direction is None else direction + d
        magnitude = m if magnitude is None else magnitude + m
    return direction * jnp.exp(0.5 * jnp.tanh(magnitude))


def pieces_of(own):
    strips = own // STRIP
    return max(k for k in range(1, MOST + 1) if strips % k == 0)


class Plan:
    def __init__(self, n_dp, n_mp, own):
        self.n, self.m, self.own = n_dp, n_mp, own
        self.k = pieces_of(own)
        self.pr = own // self.k
        self.lag = min(LAG, self.k)
        self.late = (2 * n_dp - 1) * self.k + max(0, self.lag + 8 - self.k)
        self.nt = self.late + self.k
        s0 = (n_dp - 2) * self.k + self.lag
        self.stats = (s0, s0 + (n_dp - 1) * self.k)
        self.send1 = tuple(s + self.k for s in self.stats)
        self.send2 = tuple(s + 2 for s in self.send1)
        self.done = tuple(s + 4 for s in self.send2)
        self.params = tuple(s + 1 for s in self.done)
        self.gathered = (2 * n_dp - 1) * self.k + self.lag * (n_dp - 1)
        self.end = max(self.nt + self.lag * (n_dp - 1) + DEPTH, self.params[1] + self.k + 1)


def either(T, ticks):
    return (T == ticks[0]) | (T == ticks[1]), jnp.where(T >= ticks[1], 1, 0)


def within(T, starts, length):
    t = jnp.where(T >= starts[1], 1, 0)
    k = T - jnp.where(T >= starts[1], starts[1], starts[0])
    return (k >= 0) & (k < length), t, jnp.clip(k, 0, length - 1)


def mega_kernel(
    plan, feats, hidden,
    grad_ref, master_ref, mom_ref, sec_ref, step_ref, first_ref, bias_ref, second_ref, weight_ref,
    full_ref, p1_ref, right_ref, left_ref, g_ref, coef,
    gbuf, rbuf, masters, moms, secs, fbuf, pbuf, acc, tot, near, nsum, far,
    load_sem, state_sem, send_sem, recv_sem, near_s, near_r, far_s, far_r, out_sem,
):
    n, m_n, own, K, pr = plan.n, plan.m, plan.own, plan.k, plan.pr
    width = (feats + 3) * hidden
    z = lax.axis_index("dp")
    m = lax.axis_index("mp")
    sides = (right_ref, left_ref)

    def landing(d, receiver):
        first = (receiver < n // 2) == (d == 0) if n == 4 else jnp.bool_(d == 0)
        return first, ~first

    def chunk_load(t, c):
        rows = pl.ds(pl.multiple_of(c * own, STRIP), own)
        return pltpu.make_async_copy(grad_ref.at[0, 0, t, rows], gbuf.at[t, rows], load_sem.at[t, c])

    def state_loads(t):
        return (
            pltpu.make_async_copy(master_ref.at[0, t], masters.at[t], state_sem.at[t, 0]),
            pltpu.make_async_copy(mom_ref.at[:, 0, t], moms.at[t], state_sem.at[t, 1]),
            pltpu.make_async_copy(sec_ref.at[:, 0, t], secs.at[t], state_sem.at[t, 2]),
        )

    order = []
    for i in range((n + 1) // 2):
        order += [n - 1 - i] + ([i] if i != n - 1 - i else [])
    for c in order[:2]:
        chunk_load(0, c).start()

    barrier = pltpu.get_barrier_semaphore()
    for j in range(1, m_n):
        pl.semaphore_signal(barrier, inc=1, device_id=(z, lax.rem(m + j, m_n)), device_id_type=MESH)
    for j in range(1, n):
        pl.semaphore_signal(barrier, inc=1, device_id=(lax.rem(z + j, n), m), device_id_type=MESH)
    pl.semaphore_wait(barrier, m_n - 1 + n - 1)

    def place_of(d, T):
        q = z if d == 0 else n - 1 - z
        tau = T - plan.lag * q
        active = (tau >= 0) & (tau < plan.nt)
        tau = jnp.clip(tau, 0, plan.nt - 1)
        late = tau >= plan.late
        active = active & (late | (tau < (2 * n - 1) * K))
        s, k = lax.div(tau, K), lax.rem(jnp.where(late, tau - plan.late, tau), K)
        mid = (s >= n - 1) & (tau < (2 * n - 1) * K)
        cp = jnp.where(mid, 2 * n - 2 - s, jnp.where(late, q, n - 1 - s))
        t = jnp.where(mid, 1, 0)
        c = cp if d == 0 else n - 1 - cp
        si = jnp.clip(n - 1 - cp, 0, n - 2)
        return q, tau, active, k, mid, late, cp, t, c, si

    def piece(base, k):
        return pl.ds(pl.multiple_of(base + k * pr, STRIP), pr)

    def remote(d, src, dst, tau):
        to = lax.rem(z + 1, n) if d == 0 else lax.rem(z + n - 1, n)
        return pltpu.make_async_remote_copy(
            src_ref=src, dst_ref=dst, send_sem=send_sem.at[d, lax.rem(tau, DEPTH)], recv_sem=recv_sem.at[d, tau],
            device_id=(to, m), device_id_type=MESH,
        )

    def tick(T, carry):
        for d in range(2):
            q, tau, active, k, mid, late, cp, t, c, si = place_of(d, T)
            slot = rbuf.at[d, t, si, piece(0, k)]
            landed = fbuf.at[piece(c * own, k)]

            @pl.when(active & (q > 0) & (cp >= q) & ~late)
            def _():
                remote(d, slot, slot, tau).wait_recv()

            @pl.when(active & mid & (cp < q))
            def _():
                remote(d, landed, landed, tau).wait_recv()

            for side, chosen in enumerate(landing(d, z)):

                @pl.when(active & late & (q > 0) & chosen)
                def _():
                    remote(d, sides[side].at[piece(0, k)], sides[side].at[piece(0, k)], tau).wait_recv()

            @pl.when(active & (cp > q) & (k == 0))
            def _():
                chunk_load(t, c).wait()

            @pl.when(active & (q > 0) & (cp > q))
            def _():
                rows = piece(0, k)
                rbuf[d, t, si, rows, :] = rbuf[d, t, si, rows, :] + gbuf[t, piece(c * own, k), :]

        for d in range(2):
            q, tau, active, k, mid, late, cp, t, c, si = place_of(d, T - DEPTH)
            slot = rbuf.at[d, t, si, piece(0, k)]

            @pl.when(active & (q < n - 1) & ((cp > q) | mid | late))
            def _():
                remote(d, slot, slot, tau).wait_send()

            q, tau, active, k, mid, late, cp, t, c, si = place_of(d, T)
            slot = rbuf.at[d, t, si, piece(0, k)]
            landed = fbuf.at[piece(c * own, k)]

            @pl.when(active & (cp > q) & (q == 0))
            def _():
                remote(d, gbuf.at[t, piece(c * own, k)], slot, tau).start()

            @pl.when(active & (cp > q) & (q > 0))
            def _():
                remote(d, slot, slot, tau).start()

            @pl.when(active & mid & (cp <= q) & (q < n - 1))
            def _():
                remote(d, landed, landed, tau).start()

            for side, chosen in enumerate(landing(d, z + 1 if d == 0 else z - 1)):

                @pl.when(active & late & (q < n - 1) & chosen)
                def _():
                    remote(d, pbuf.at[piece(0, k)], sides[side].at[piece(0, k)], tau).start()

        @pl.when(T == 0)
        def _():
            for c in order[2:]:
                chunk_load(0, c).start()
            for c in order:
                chunk_load(1, c).start()

        for t in range(2):

            @pl.when(T == 2 + 2 * t)
            def _():
                for copy in state_loads(t):
                    copy.start()

        for d in range(2):
            edge = 0 if d == 0 else n - 1

            @pl.when((z == edge) & (T < K))
            def _():
                rows = piece(0, jnp.minimum(T, K - 1))
                for t in range(2):
                    rbuf[d, t, n - 2, rows, :] = jnp.zeros((pr, 128), jnp.bfloat16)

        live, t, k = within(T, plan.stats, K)

        @pl.when(live & (k == 0))
        def _():
            for copy in state_loads(t):
                copy.wait()
            chunk_load(t, z).wait()
            acc[...] = jnp.zeros_like(acc)

        @pl.when(live)
        def _():
            side = [jnp.minimum(n - 1 - z, n - 2), jnp.minimum(z, n - 2)]

            def body(i, sums):
                rows = pl.ds(pl.multiple_of(k * pr + i * STRIP, STRIP), STRIP)
                mine = pl.ds(pl.multiple_of(z * own + k * pr + i * STRIP, STRIP), STRIP)
                g = gbuf[t, mine, :].astype(jnp.float32)
                for d in range(2):
                    g = g + rbuf[d, t, side[d], rows, :].astype(jnp.float32)
                g = g.astype(jnp.bfloat16)
                gbuf[t, mine, :] = g
                g = g.astype(jnp.float32)
                moments, squares = advanced(
                    g, [moms[t, c, rows, :] for c in range(3)], [secs[t, c, rows, :] for c in range(3)]
                )
                listing = listing_of(masters[t, rows, :], g, moments, squares)
                return tuple(
                    a + jnp.sum((f * f).reshape(STRIP // 8, 8, 128), axis=0) for a, f in zip(sums, listing)
                )

            sums = lax.fori_loop(0, pr // STRIP, body, tuple(acc[f] for f in range(8)))
            for f in range(8):
                acc[f] = sums[f]

        @pl.when(live & (k == K - 1))
        def _():
            for f in range(8):
                tot[t, pl.ds(f, 1), :] = jnp.sum(acc[f], axis=0, keepdims=True)

        def near_copy(t, j):
            return pltpu.make_async_remote_copy(
                src_ref=tot.at[t], dst_ref=near.at[t, j], send_sem=near_s.at[t, j], recv_sem=near_r.at[t, j],
                device_id=(z, lax.rem(m + j, m_n)), device_id_type=MESH,
            )

        def far_copy(t, j):
            return pltpu.make_async_remote_copy(
                src_ref=nsum.at[t], dst_ref=far.at[t, j], send_sem=far_s.at[t, j], recv_sem=far_r.at[t, j],
                device_id=(lax.rem(z + j, n), m), device_id_type=MESH,
            )

        live, t = either(T, plan.send1)

        @pl.when(live)
        def _():
            for j in range(1, m_n):
                near_copy(t, j).start()

        live, t = either(T, tuple(s - 1 for s in plan.send2))

        @pl.when(live)
        def _():
            for j in range(1, m_n):
                near_copy(t, j).wait()
            total = tot[t]
            for j in range(1, m_n):
                total = total + near[t, j]
            nsum[t] = total

        live, t = either(T, plan.send2)

        @pl.when(live)
        def _():
            for j in range(1, n):
                far_copy(t, j).start()

        live, t = either(T, plan.done)

        @pl.when(live)
        def _():
            for j in range(1, n):
                far_copy(t, j).wait()
            total = nsum[t]
            for j in range(1, n):
                total = total + far[t, j]
            base = t * width
            sums = jnp.sum(total, axis=1, keepdims=True) + jnp.zeros((feats, 128), jnp.float32)
            norms = jnp.sqrt(sums / float(m_n * n * own * 128) + 1e-06)
            logs = jnp.log(norms)
            inverse = 1.0 / norms
            step = jnp.full((1, 128), step_ref[0].astype(jnp.float32))
            logits = weight_ref[feats] * (jnp.log(1.0 + step) / 11.5) + weight_ref[feats + 1] * (step / 100000.0)
            for f in range(feats):
                logits = logits + weight_ref[f] * logs[f : f + 1, :]
            boost = jnp.exp(jnp.tanh(logits))[0, 0]
            for f in range(feats):
                scale = inverse[f, 0]
                for j in range(hidden):
                    coef[base + f * hidden + j] = first_ref[j, f] * scale
            tail = base + feats * hidden
            for j in range(hidden):
                coef[tail + j] = bias_ref[j]
                coef[tail + hidden + j] = second_ref[0, j] * boost
                coef[tail + 2 * hidden + j] = second_ref[1, j]

        live, t, k = within(T, plan.params, K)

        def params(fresh, at):
            def body(i, carry):
                rows = pl.ds(pl.multiple_of(k * pr + i * STRIP, STRIP), STRIP)
                mine = pl.ds(pl.multiple_of(z * own + k * pr + i * STRIP, STRIP), STRIP)
                g = gbuf[t, mine, :].astype(jnp.float32)
                moments, squares = advanced(
                    g, [moms[t, c, rows, :] for c in range(3)], [secs[t, c, rows, :] for c in range(3)]
                )
                master = masters[t, rows, :]
                update = update_of(listing_of(master, g, moments, squares), coef, t * width, feats, hidden)
                to = pl.ds(pl.multiple_of(at + k * pr + i * STRIP, STRIP), STRIP)
                fresh[to, :] = (master - 0.05 * update).astype(jnp.bfloat16)
                return carry

            lax.fori_loop(0, pr // STRIP, body, 0)

        @pl.when(live & (t == 0))
        def _():
            params(fbuf, z * own)

        @pl.when(live & (t == 1))
        def _():
            params(pbuf, 0)

        @pl.when(T == plan.gathered)
        def _():
            out(0).start()

        @pl.when(T == plan.params[1] + K)
        def _():
            out(3).start()

        for t in range(2):

            @pl.when(T == plan.stats[t] + K)
            def _():
                out(1 + t).start()

        return carry

    def out(i):
        mine = pl.ds(pl.multiple_of(z * own, STRIP), own)
        src, dst = (
            (fbuf, full_ref),
            (gbuf.at[0, mine], g_ref.at[0]),
            (gbuf.at[1, mine], g_ref.at[1]),
            (pbuf, p1_ref),
        )[i]
        return pltpu.make_async_copy(src, dst, out_sem.at[i])

    lax.fori_loop(0, plan.end, tick, 0)
    for i in range(4):
        out(i).wait()


def mega(n_dp, n_mp, grad_parts, master, momenta, second, step_count, mlp_first, mlp_bias, mlp_second, tensor_weight):
    feats, hidden = mlp_first.shape
    own, total_rows = master.shape[2], grad_parts.shape[3]
    plan = Plan(n_dp, n_mp, own)
    width = (feats + 3) * hidden
    smem = pl.BlockSpec(memory_space=pltpu.SMEM)
    anywhere = pl.BlockSpec(memory_space=pl.ANY)
    sem = pltpu.SemaphoreType.DMA
    return pl.pallas_call(
        functools.partial(mega_kernel, plan, feats, hidden),
        out_shape=(
            jax.ShapeDtypeStruct((total_rows, 128), jnp.bfloat16),
            jax.ShapeDtypeStruct((own, 128), jnp.bfloat16),
            jax.ShapeDtypeStruct((own, 128), jnp.bfloat16),
            jax.ShapeDtypeStruct((own, 128), jnp.bfloat16),
            jax.ShapeDtypeStruct((2, own, 128), jnp.bfloat16),
            jax.ShapeDtypeStruct((2 * width,), jnp.float32),
        ),
        in_specs=[anywhere] * 4 + [smem] * 5,
        out_specs=(anywhere,) * 5 + (smem,),
        scratch_shapes=[
            pltpu.VMEM((2, total_rows, 128), jnp.bfloat16),
            pltpu.VMEM((2, 2, n_dp - 1, own, 128), jnp.bfloat16),
            pltpu.VMEM((2, own, 128), jnp.float32),
            pltpu.VMEM((2, 3, own, 128), jnp.float32),
            pltpu.VMEM((2, 3, own, 128), jnp.float32),
            pltpu.VMEM((total_rows, 128), jnp.bfloat16),
            pltpu.VMEM((own, 128), jnp.bfloat16),
            pltpu.VMEM((8, 8, 128), jnp.float32),
            pltpu.VMEM((2, feats, 128), jnp.float32),
            pltpu.VMEM((2, n_mp, feats, 128), jnp.float32),
            pltpu.VMEM((2, feats, 128), jnp.float32),
            pltpu.VMEM((2, n_dp, feats, 128), jnp.float32),
            sem((2, n_dp)),
            sem((2, 3)),
            sem((2, DEPTH)),
            sem((2, plan.nt)),
            sem((2, n_mp)),
            sem((2, n_mp)),
            sem((2, n_dp)),
            sem((2, n_dp)),
            sem((4,)),
        ],
        compiler_params=pltpu.CompilerParams(
            collective_id=0, has_side_effects=True, vmem_limit_bytes=67_000_000
        ),
        cost_estimate=pl.CostEstimate(flops=10**9, bytes_accessed=10**8, transcendentals=0),
        name="exchange",
    )(grad_parts, master, momenta, second, step_count, mlp_first.T, mlp_bias, mlp_second.T, tensor_weight)


def finish_kernel(t, feats, hidden, width, coef, g_ref, master_ref, mom_ref, sec_ref, *rest):
    nm_ref, nmom_ref, nsec_ref, up_ref = rest[-4:]
    part = 64 if g_ref.shape[1] % 64 == 0 else STRIP

    def body(k, carry):
        rows = pl.ds(pl.multiple_of(k * part, part), part)
        g = g_ref[0, rows, :].astype(jnp.float32)
        moments, squares = advanced(
            g, [mom_ref[c, 0, 0, rows, :] for c in range(3)], [sec_ref[c, 0, 0, rows, :] for c in range(3)]
        )
        for c in range(3):
            nmom_ref[c, 0, 0, rows, :] = moments[c]
            nsec_ref[c, 0, 0, rows, :] = squares[c]
        master = master_ref[0, 0, rows, :]
        update = update_of(listing_of(master, g, moments, squares), coef, t * width, feats, hidden)
        up_ref[0, 0, rows, :] = update
        nm_ref[0, 0, rows, :] = master - 0.05 * update
        return carry

    lax.fori_loop(0, g_ref.shape[1] // part, body, 0)


def finish(t, feats, hidden, coefs, g, master, momenta, second, earlier=()):
    own = g.shape[1]
    rows = block_rows(own, BLOCK)
    specs = [
        pl.BlockSpec((1, 1, rows, 128), lambda i: (0, t, i, 0)),
        pl.BlockSpec((3, 1, 1, rows, 128), lambda i: (0, 0, t, i, 0)),
        pl.BlockSpec((3, 1, 1, rows, 128), lambda i: (0, 0, t, i, 0)),
    ]
    return pl.pallas_call(
        functools.partial(finish_kernel, t, feats, hidden, coefs.shape[0] // 2),
        grid=(own // rows,),
        out_shape=(
            jax.ShapeDtypeStruct(master.shape, jnp.float32),
            jax.ShapeDtypeStruct(momenta.shape, jnp.float32),
            jax.ShapeDtypeStruct(second.shape, jnp.float32),
            jax.ShapeDtypeStruct(master.shape, jnp.float32),
        ),
        in_specs=[
            pl.BlockSpec(memory_space=pltpu.SMEM),
            pl.BlockSpec((1, rows, 128), lambda i: (t, i, 0)),
        ]
        + specs
        + [pl.BlockSpec(memory_space=pl.ANY)] * len(earlier),
        out_specs=(specs[0], specs[1], specs[2], specs[0]),
        input_output_aliases={5 + i: i for i in range(len(earlier))},
        cost_estimate=pl.CostEstimate(
            flops=own * 128 * 130, bytes_accessed=own * 128 * 62, transcendentals=5 * own * 128
        ),
        name=f"finish{t}",
    )(coefs, g, master, momenta, second, *earlier)


def assemble_kernel(n_dp, own, chunks, full_ref, mine_ref, *rest):
    count = len(chunks)
    others = rest[:count]
    out_ref, fbuf, buf, load_sem, store_sem = rest[count:]
    z = lax.axis_index("dp")
    moves = [(full_ref, fbuf, out_ref.at[0, 0], None)]
    moves.append((mine_ref, buf.at[0], out_ref.at[0, 1, pl.ds(pl.multiple_of(z * own, STRIP), own)], None))
    for i, chunk in enumerate(chunks):
        c = chunk(z)
        at = pl.ds(pl.multiple_of(jnp.clip(c, 0, n_dp - 1) * own, STRIP), own)
        moves.append((others[i], buf.at[1 + i], out_ref.at[0, 1, at], (c >= 0) & (c < n_dp)))

    def each(act):
        for i, (src, mid, dst, ok) in enumerate(moves):
            def move(i=i, src=src, mid=mid, dst=dst):
                act(
                    functools.partial(pltpu.make_async_copy, src, mid, load_sem.at[i]),
                    functools.partial(pltpu.make_async_copy, mid, dst, store_sem.at[i]),
                )

            if ok is None:
                move()
            else:
                pl.when(ok)(move)

    each(lambda load, store: load().start())

    def forward(load, store):
        load().wait()
        store().start()

    each(forward)
    each(lambda load, store: store().wait())


def assemble(n_dp, full, mine, others, chunks):
    own = mine.shape[0]
    anywhere = pl.BlockSpec(memory_space=pl.ANY)
    count = 2 + len(others)
    return pl.pallas_call(
        functools.partial(assemble_kernel, n_dp, own, chunks),
        out_shape=jax.ShapeDtypeStruct((1, 2) + full.shape, full.dtype),
        in_specs=[anywhere] * count,
        out_specs=anywhere,
        scratch_shapes=[
            pltpu.VMEM(full.shape, full.dtype),
            pltpu.VMEM((count - 1,) + mine.shape, mine.dtype),
            pltpu.SemaphoreType.DMA((count,)),
            pltpu.SemaphoreType.DMA((count,)),
        ],
        cost_estimate=pl.CostEstimate(flops=10**7, bytes_accessed=4 * full.size, transcendentals=0),
        name="assemble",
    )(full, mine, *others)


def last_kernel(n_dp, own, *rest):
    out_ref, sem = rest[-2:]
    z = lax.axis_index("dp")
    for i, row in enumerate((0, (n_dp - 1) * own)):

        @pl.when(z == (n_dp - 1 if i == 0 else 0))
        def _():
            src = rest[0] if i == 0 else rest[len(rest) - 4]
            store = pltpu.make_async_copy(src, out_ref.at[0, 1, pl.ds(row, own)], sem)
            store.start()
            store.wait()


def last(n_dp, arrived, out):
    anywhere = pl.BlockSpec(memory_space=pl.ANY)
    return pl.pallas_call(
        functools.partial(last_kernel, n_dp, arrived[0].shape[0]),
        out_shape=jax.ShapeDtypeStruct(out.shape, out.dtype),
        in_specs=[anywhere] * (len(arrived) + 1),
        out_specs=anywhere,
        input_output_aliases={len(arrived): 0},
        scratch_shapes=[pltpu.SemaphoreType.DMA],
        compiler_params=pltpu.CompilerParams(vmem_limit_bytes=4 << 20),
        name="last",
    )(*arrived, out)


def local(
    n_dp, n_mp, grad_parts, master, momenta, second, step_count, mlp_first, mlp_bias, mlp_second, tensor_weight
):
    feats, hidden = mlp_first.shape
    full0, p1, right, left, g, coefs = mega(
        n_dp, n_mp, grad_parts, master, momenta, second, step_count, mlp_first, mlp_bias, mlp_second, tensor_weight
    )
    others = [right, left]
    net = (feats, hidden, coefs, g, master, momenta, second)
    if n_dp == 4:
        inner, outer = right, left
        crossed = lax.ppermute(inner, "dp", [(1, 2), (2, 1)])
        ended = lax.ppermute(outer, "dp", [(2, 3), (1, 0)])
        state = finish(0, *net)
        crossed, state = lax.optimization_barrier((crossed, state))
        arrived = [lax.ppermute(crossed, "dp", [(2, 3), (1, 0)])]
        state = finish(1, *net, state)
        others += [crossed, ended]
        none = -1
        chunks = [
            lambda z: jnp.where(z == 1, 0, jnp.where(z == 2, 3, none)),
            lambda z: jnp.where(z < 2, z + 1, z - 1),
            lambda z: jnp.where(z == 1, 3, jnp.where(z == 2, 0, none)),
            lambda z: jnp.where(z == 0, 2, jnp.where(z == 3, 1, none)),
        ]
    else:
        chunks = [lambda z: z - 1, lambda z: z + 1]
        state = ()
        for step in range(2, n_dp):
            sent = (right, left)
            right = lax.ppermute(sent[0], "dp", [(i, i + 1) for i in range(step - 1, n_dp - 1)])
            left = lax.ppermute(sent[1], "dp", [(i, i - 1) for i in range(1, n_dp - step + 1)])
            if step <= 3:
                state = finish(step - 2, *net, state)
            if step < n_dp - 1:
                right, left, state = lax.optimization_barrier((right, left, state))
                others += [right, left]
                chunks += [lambda z, step=step: z - step, lambda z, step=step: z + step]
        arrived = [right, left]
    out = last(n_dp, arrived, assemble(n_dp, full0, p1, others, chunks))
    return (out, *state)


def solution(mesh):
    placed = (
        P("dp", "mp", None, None, None),
        P("mp", None, "dp", None),
        P(None, "mp", None, "dp", None),
        P(None, "mp", None, "dp", None),
        P(),
        P(),
        P(),
        P(),
        P(),
    )
    return jax.shard_map(
        functools.partial(local, mesh.shape["dp"], mesh.shape["mp"]),
        mesh=mesh,
        in_specs=placed,
        out_specs=(
            P("mp", None, None, None),
            P("mp", None, "dp", None),
            P(None, "mp", None, "dp", None),
            P(None, "mp", None, "dp", None),
            P("mp", None, "dp", None),
        ),
        check_vma=False,
    )
```
